32 devices in a mesh: grp: 4 (over y, x), grid: 8 (over z, core).
Axes of the slice: x: 2, y: 2, z: 4, core: 2. Of those that a mesh axis runs over, the one named last changes fastest.
Arguments:
- orbitals: float32 [64, 262144], P('grp', 'grid'), may hold values from -6 to 6
- anchors: int32 [64, 3], replicated, may hold values from 0 to 31
- pair_slots: int32 [32, 4, 2], replicated, may hold values from -1 to 63, as said below
Outputs:
- exchange_term: float32 [64, 262144], P('grp', 'grid')
The draws below stay inside these ranges and needn't reach their ends.
Inputs may be any that keep to these rules, and one draw needn't show every extreme that they name: `pair_slots`: row k lists the pairs of owner k, the device with index k in the order grp, grid; its first slots hold pairs of two different orbital numbers and its other slots hold -1 in both columns. Exactly 64 slots hold pairs in all, no row holds more than 4, and some row holds exactly 4.
All inputs are finite; a program needn't handle non-finite values.
Results may differ from the reference program's by a relative error of at most 0.0003.
Values sent between devices are 32-bit elements; how exact they have to be, the bound alone decides.
A program may use at most 128 MiB of HBM per device.

```python
import jax
import jax.numpy as jnp
from jax import lax

B = 64
PAIR_DEV = 2
ITERS = 3
OWNERS = 32
NORB = 64
CAP = 4


def draw_pair_slots(key, part):
    order_key, first_key, gap_key = jax.random.split(jax.random.fold_in(key, 7), 3)
    position = jnp.argsort(jax.random.permutation(order_key, OWNERS))
    load = jnp.where(position < OWNERS // 4, CAP, jnp.where(position < 3 * OWNERS // 4, PAIR_DEV, 0))
    slot_idx = lax.broadcasted_iota(jnp.int32, (OWNERS, CAP), 1)
    filled = slot_idx < load[:, None]
    orbit_a = jax.random.randint(first_key, (OWNERS, CAP), 0, NORB)
    orbit_b = (orbit_a + jax.random.randint(gap_key, (OWNERS, CAP), 1, NORB)) % NORB
    paired = jnp.stack([orbit_a, orbit_b], -1)
    return jnp.where(filled[..., None], paired, -1).astype(jnp.int32)


def plant(drawn, stream_key, least, largest):
    place = [jax.random.randint(jax.random.fold_in(stream_key, axis), (), 0, length) for axis, length in enumerate(drawn.shape)]
    widest = drawn.shape.index(max(drawn.shape))
    next_to = place[:widest] + [(place[widest] + 1) % drawn.shape[widest]] + place[widest + 1:]
    return drawn.at[tuple(place)].set(least).at[tuple(next_to)].set(largest)


def block_scale(stream_key, dims, cuts, smallest, high):
    factor_of = 1.0
    for axis_at, parts in cuts:
        steps = jax.random.uniform(jax.random.fold_in(jax.random.fold_in(stream_key, 6), axis_at), (parts,), jnp.float32, smallest / len(cuts), high / len(cuts))
        factor_of = factor_of * jnp.repeat(jnp.exp(steps), dims[axis_at] // parts).reshape((-1,) + (1,) * (len(dims) - 1 - axis_at))
    return factor_of


def normal_values(key, shape, width, limit, cuts=(), kind=jnp.bfloat16):
    level = block_scale(key, shape, cuts, -0.22, 0.18) if cuts else 1.0
    values = jax.random.normal(key, shape, jnp.float32) * width * level
    return jnp.minimum(jnp.maximum(values, -limit), limit).astype(kind)


def setup_inputs(seed: int = 0) -> dict:
    keys = jax.random.split(jax.random.key(seed), 4)
    return {
        "orbitals": normal_values(keys[0], (NORB, B * B * B), 1.0, 6.0, ((0, 4), (1, 8)), jnp.float32),
        "anchors": plant(jax.random.randint(keys[1], (NORB, 3), 0, B // 2), jax.random.fold_in(keys[1], 1), 0, (B // 2) - 1).astype(jnp.int32),
        "pair_slots": draw_pair_slots(jax.random.fold_in(keys[3], 71), 0),
    }


def shift_field(field, offset, extent):
    plane_size = extent * extent
    padded_x = jnp.pad(field, ((extent, extent), (0, 0)))
    moved = lax.dynamic_slice_in_dim(padded_x, (extent - offset[0]).astype(jnp.int32), extent, 0)
    padded_yz = jnp.pad(moved, ((0, 0), (plane_size, plane_size)))
    linear = (offset[1] * extent + offset[2]).astype(jnp.int32)
    moved = lax.dynamic_slice_in_dim(padded_yz, (plane_size - linear).astype(jnp.int32), plane_size, 1)
    cells = lax.broadcasted_iota(jnp.int32, (1, plane_size), 1)
    coord_y = cells // extent - offset[1]
    coord_z = cells % extent - offset[2]
    inside = (coord_y >= 0) & (coord_y < extent) & (coord_z >= 0) & (coord_z < extent)
    return jnp.where(inside, moved, jnp.zeros_like(moved))


def operate(field, extent):
    padded_x = jnp.pad(field, ((1, 1), (0, 0)))
    beside = padded_x[2:] + padded_x[:-2]
    padded_y = jnp.pad(field, ((0, 0), (extent, extent)))
    beside = beside + padded_y[:, 2 * extent:] + padded_y[:, :-2 * extent]
    padded_z = jnp.pad(field, ((0, 0), (1, 1)))
    cells = lax.broadcasted_iota(jnp.int32, (1, field.shape[1]), 1) % extent
    upper_z = jnp.where(cells < extent - 1, padded_z[:, 2:], jnp.zeros_like(field))
    lower_z = jnp.where(cells > 0, padded_z[:, :-2], jnp.zeros_like(field))
    return 6.0 * field - beside - upper_z - lower_z


def conjugate(density, extent):
    potential = jnp.zeros_like(density)
    resid = density
    direction = density
    norm_now = jnp.sum(resid * resid)
    for turn in range(ITERS):
        image = operate(direction, extent)
        step_len = norm_now / jnp.sum(direction * image)
        potential = potential + step_len * direction
        resid = resid - step_len * image
        norm_next = jnp.sum(resid * resid)
        direction = resid + (norm_next / norm_now) * direction
        norm_now = norm_next
    return potential


def pair_terms(field_a, field_b, offset, extent):
    partner = shift_field(field_b, offset, extent)
    density = field_a * partner
    potential = conjugate(density, extent)
    term_a = potential * partner
    term_b = shift_field(potential * field_a, -offset, extent)
    return term_a, term_b


def reference(orbitals, anchors, pair_slots):
    extent = B
    slot_list = pair_slots.reshape(-1, 2)

    def add_pair(accum, slot_entry):
        filled = slot_entry[0] >= 0
        orbit_a = jnp.maximum(slot_entry[0], 0).astype(jnp.int32)
        orbit_b = jnp.maximum(slot_entry[1], 0).astype(jnp.int32)
        offset = anchors[orbit_b] - anchors[orbit_a]
        field_a = orbitals[orbit_a].reshape(extent, extent * extent)
        field_b = orbitals[orbit_b].reshape(extent, extent * extent)
        term_a, term_b = pair_terms(field_a, field_b, offset, extent)
        weight_flag = jnp.where(filled, 1.0, 0.0).astype(orbitals.dtype)
        accum = accum.at[orbit_a].add(weight_flag * term_a.reshape(-1))
        accum = accum.at[orbit_b].add(weight_flag * term_b.reshape(-1))
        return accum, None

    start = jnp.zeros(orbitals.shape, orbitals.dtype)
    accum, unused = lax.scan(add_pair, start, slot_list)
    return accum
```

```python
import math

import jax
import jax.numpy as jnp
from jax import lax
from jax.experimental import pallas as pl
from jax.experimental.pallas import tpu as pltpu
from jax.sharding import PartitionSpec as P

B = 64
PAIR_DEV = 2
ITERS = 3
MOST_CHUNKS = 2
LANES = 128
ROWS = B * B // LANES
PAD = 32
STEP = 4


def deal_evenly(pair_slots, owner_count, each_owner):
    flat_slots = pair_slots.reshape(-1, 2)
    filled = (flat_slots[:, 0] >= 0).astype(jnp.int32)
    position = jnp.cumsum(filled, dtype=jnp.int32) - filled
    wanted = lax.broadcasted_iota(jnp.int32, (owner_count, each_owner), 1) * owner_count
    wanted = (wanted + lax.broadcasted_iota(jnp.int32, (owner_count, each_owner), 0)).reshape(-1)
    matched = (position[None, :] == wanted[:, None]) & (filled[None, :] == 1)
    picked = jnp.sum(jnp.where(matched[:, :, None], flat_slots[None], 0), axis=1)
    return picked.reshape(owner_count, each_owner, 2)


def gather_kernel(ids_ref, src_ref, *out_refs):
    count, terms = out_refs[0].shape[:2]
    for slot, out_ref in enumerate(out_refs):
        def pick(dest, unused, slot=slot, out_ref=out_ref):
            for term in range(terms):
                out_ref[dest, term] = src_ref[ids_ref[(slot * count + dest) * terms + term]]
            return unused

        lax.fori_loop(0, count, pick, 0)


def gather_pieces(ids, pieces, slots, count):
    norb, rows, lanes = pieces.shape
    block = max(8, rows // 4)
    return pl.pallas_call(
        gather_kernel,
        grid_spec=pltpu.PrefetchScalarGridSpec(
            num_scalar_prefetch=1,
            grid=(rows // block,),
            in_specs=[pl.BlockSpec((norb, block, lanes), lambda i, ids: (0, i, 0))],
            out_specs=[pl.BlockSpec((count, 2, block, lanes), lambda i, ids: (0, 0, i, 0))] * slots,
        ),
        out_shape=[jax.ShapeDtypeStruct((count, 2, rows, lanes), jnp.float32)] * slots,
        cost_estimate=pl.CostEstimate(flops=0, bytes_accessed=8 * norb * rows * lanes, transcendentals=0),
        name="pick_pieces",
    )(ids, pieces)


def scatter_kernel(ids_ref, *refs):
    out_ref = refs[-1]
    out_ref[...] = jnp.zeros_like(out_ref)
    count, terms = refs[0].shape[:2]
    for slot, in_ref in enumerate(refs[:-1]):
        def add(dest, unused, slot=slot, in_ref=in_ref):
            for term in range(terms):
                orbit = ids_ref[(slot * count + dest) * terms + term]
                out_ref[orbit] = out_ref[orbit] + in_ref[dest, term]
            return unused

        lax.fori_loop(0, count, add, 0)


def scatter_pieces(ids, parts, norb):
    count, terms, rows, lanes = parts[0].shape
    block = max(8, rows // 4)
    return pl.pallas_call(
        scatter_kernel,
        grid_spec=pltpu.PrefetchScalarGridSpec(
            num_scalar_prefetch=1,
            grid=(rows // block,),
            in_specs=[pl.BlockSpec((count, terms, block, lanes), lambda i, ids: (0, 0, i, 0))] * len(parts),
            out_specs=pl.BlockSpec((norb, block, lanes), lambda i, ids: (0, i, 0)),
        ),
        out_shape=jax.ShapeDtypeStruct((norb, rows, lanes), jnp.float32),
        cost_estimate=pl.CostEstimate(flops=0, bytes_accessed=8 * norb * rows * lanes, transcendentals=0),
        name="add_pieces",
    )(ids, *parts)


def lane_ids(shape):
    return lax.broadcasted_iota(jnp.int32, shape, len(shape) - 1)


def shift_plane(plane, off_y, off_z):
    shape = plane.shape
    lane = lane_ids(shape)
    row = lax.broadcasted_iota(jnp.int32, shape, 0)
    linear = off_y * B + off_z
    across = jnp.bitwise_and(linear, LANES - 1)
    down = jnp.right_shift(linear, 7)
    turned = pltpu.roll(plane, across, 1)
    near = pltpu.roll(turned, jnp.bitwise_and(down, ROWS - 1), 0)
    far = pltpu.roll(turned, jnp.bitwise_and(down + 1, ROWS - 1), 0)
    moved = jnp.where(lane >= across, near, far)
    from_y = row * 2 + jnp.right_shift(lane, 6) - off_y
    from_z = jnp.bitwise_and(lane, B - 1) - off_z
    inside = (from_y >= 0) & (from_y < B) & (from_z >= 0) & (from_z < B)
    return jnp.where(inside, moved, 0.0)


def operate_plane(before, plane, after):
    shape = plane.shape
    lane = lane_ids(shape)
    row = lax.broadcasted_iota(jnp.int32, shape, 0)
    z = jnp.bitwise_and(lane, B - 1)
    upper_z = jnp.where(z < B - 1, pltpu.roll(plane, LANES - 1, 1), 0.0)
    lower_z = jnp.where(z > 0, pltpu.roll(plane, 1, 1), 0.0)
    half = pltpu.roll(plane, B, 1)
    down = jnp.where(row > 0, pltpu.roll(half, 1, 0), 0.0)
    up = jnp.where(row < ROWS - 1, pltpu.roll(half, ROWS - 1, 0), 0.0)
    beside = (before + after) + (half + jnp.where(lane < B, down, up))
    return 6.0 * plane - beside - upper_z - lower_z


def fold(values):
    return jnp.sum(values.reshape(ROWS // 8, 8, LANES), axis=0)


def total(acc):
    return jnp.sum(acc, axis=(0, 1), keepdims=True)


def solve_kernel(info_ref, *refs):
    chunks = (len(refs) - 6) // 2
    in_refs, out_refs = refs[:chunks], refs[chunks : 2 * chunks]
    wide, partner, direction, resid, image, potential = refs[2 * chunks :]
    count, terms, rows, lanes = in_refs[0].shape
    each = rows // ROWS
    dx, dy, dz = info_ref[0], info_ref[1], info_ref[2]
    keep = jnp.where(info_ref[3] > 0, 1.0, 0.0).astype(jnp.float32)
    edge = jnp.zeros((PAD, ROWS, LANES), jnp.float32)
    wide[pl.ds(0, PAD)] = edge
    wide[pl.ds(PAD + B, PAD)] = edge
    direction[0] = edge[0]
    direction[B + 1] = edge[0]
    none = jnp.zeros((8, LANES), jnp.float32)

    def place(owner, chunk, i):
        return (owner * chunks + chunk) * each + i

    def load(owner, unused):
        for chunk in range(chunks):
            for i in range(each):
                wide[PAD + place(owner, chunk, i)] = in_refs[chunk][owner, 1, pl.ds(i * ROWS, ROWS)]
        return unused

    lax.fori_loop(0, count, load, 0)

    def start(owner, acc):
        for chunk in range(chunks):
            for i in range(each):
                x = place(owner, chunk, i)
                other = shift_plane(wide[PAD + x - dx], dy, dz)
                partner[x] = other
                density = in_refs[chunk][owner, 0, pl.ds(i * ROWS, ROWS)] * other
                direction[x + 1] = density
                resid[x] = density
                acc = acc + fold(density * density)
        return acc

    norm_now = total(lax.fori_loop(0, count, start, none))

    for turn in range(ITERS):
        def apply(block, acc):
            for i in range(STEP):
                x = block * STEP + i
                plane = direction[x + 1]
                result = operate_plane(direction[x], plane, direction[x + 2])
                image[x] = result
                acc = acc + fold(plane * result)
            return acc

        step_len = norm_now / total(lax.fori_loop(0, B // STEP, apply, none))

        if turn == ITERS - 1:
            break

        def advance(block, acc):
            for i in range(STEP):
                x = block * STEP + i
                moved = step_len * direction[x + 1]
                potential[x] = moved if turn == 0 else potential[x] + moved
                left = resid[x] - step_len * image[x]
                resid[x] = left
                acc = acc + fold(left * left)
            return acc

        norm_next = total(lax.fori_loop(0, B // STEP, advance, none))
        ratio = norm_next / norm_now

        def renew(block, unused):
            for i in range(STEP):
                x = block * STEP + i
                direction[x + 1] = resid[x] + ratio * direction[x + 1]
            return unused

        lax.fori_loop(0, B // STEP, renew, 0)
        norm_now = norm_next

    def finish(owner, unused):
        for chunk in range(chunks):
            for i in range(each):
                x = place(owner, chunk, i)
                found = (potential[x] + step_len * direction[x + 1]) * keep
                out_refs[chunk][owner, 0, pl.ds(i * ROWS, ROWS)] = found * partner[x]
                wide[PAD + x] = found * in_refs[chunk][owner, 0, pl.ds(i * ROWS, ROWS)]
        return unused

    lax.fori_loop(0, count, finish, 0)

    def give_back(owner, unused):
        for chunk in range(chunks):
            for i in range(each):
                x = place(owner, chunk, i)
                out_refs[chunk][owner, 1, pl.ds(i * ROWS, ROWS)] = shift_plane(wide[PAD + x + dx], -dy, -dz)
        return unused

    lax.fori_loop(0, count, give_back, 0)


def solve_pair(info, parts):
    box = (B, ROWS, LANES)
    vmem = pl.BlockSpec(memory_space=pltpu.VMEM)
    return pl.pallas_call(
        solve_kernel,
        in_specs=[pl.BlockSpec(memory_space=pltpu.SMEM)] + [vmem] * len(parts),
        out_specs=[vmem] * len(parts),
        out_shape=[jax.ShapeDtypeStruct(p.shape, jnp.float32) for p in parts],
        scratch_shapes=[
            pltpu.VMEM((B + 2 * PAD, ROWS, LANES), jnp.float32),
            pltpu.VMEM(box, jnp.float32),
            pltpu.VMEM((B + 2, ROWS, LANES), jnp.float32),
            pltpu.VMEM(box, jnp.float32),
            pltpu.VMEM(box, jnp.float32),
            pltpu.VMEM(box, jnp.float32),
        ],
        compiler_params=pltpu.CompilerParams(vmem_limit_bytes=32 * 1024 * 1024),
        cost_estimate=pl.CostEstimate(flops=0, bytes_accessed=40 * 1024 * 1024, transcendentals=0),
        name="solve_pair",
    )(info, *parts)


def body(orbitals, anchors, pair_slots):
    grid_count = lax.axis_size("grid")
    owner_count = lax.axis_size("grp") * grid_count
    group_idx = lax.axis_index("grp")
    place_idx = lax.axis_index("grid")
    assignment = deal_evenly(pair_slots, owner_count, PAIR_DEV)
    slots = assignment.shape[1]
    filled = assignment[..., 0] >= 0
    safe_ids = jnp.maximum(assignment, 0)
    group_table = lax.dynamic_slice_in_dim(safe_ids, group_idx * grid_count, grid_count, 0)
    ids = jnp.transpose(group_table, (1, 0, 2)).reshape(-1)
    owner_idx = group_idx * grid_count + place_idx
    own_pairs = safe_ids[owner_idx]
    offsets = anchors[own_pairs[:, 1]] - anchors[own_pairs[:, 0]]
    info = jnp.concatenate([offsets, filled[owner_idx].astype(jnp.int32)[:, None]], axis=1)

    norb_local, cells = orbitals.shape
    stacked = orbitals.reshape(norb_local, cells // LANES, LANES)
    chunks = math.gcd(MOST_CHUNKS, cells // (B * B))
    rows = stacked.shape[1] // chunks
    arrived = [[None] * chunks for _ in range(slots)]
    for chunk in range(chunks):
        pieces = lax.all_gather(stacked[:, chunk * rows : (chunk + 1) * rows], "grp", axis=0, tiled=True)
        outgoing = gather_pieces(ids, pieces, slots, grid_count)
        for slot in range(slots):
            arrived[slot][chunk] = lax.all_to_all(outgoing[slot], "grid", split_axis=0, concat_axis=0, tiled=True)
    returned = []
    for slot in range(slots):
        terms = solve_pair(info[slot], arrived[slot])
        returned.append(
            [lax.all_to_all(t, "grid", split_axis=0, concat_axis=0, tiled=True) for t in terms]
        )
    results = []
    for chunk in range(chunks):
        summed = scatter_pieces(ids, [r[chunk] for r in returned], anchors.shape[0])
        results.append(lax.psum_scatter(summed, "grp", scatter_dimension=0, tiled=True))
    return jnp.concatenate(results, axis=1).reshape(norb_local, cells)


def solution(mesh):
    return jax.shard_map(
        body,
        mesh=mesh,
        in_specs=(P("grp", "grid"), P(), P()),
        out_specs=P("grp", "grid"),
        check_vma=False,
    )
```

```python
import math

import jax
import jax.numpy as jnp
from jax import lax
from jax.experimental import pallas as pl
from jax.experimental.pallas import tpu as pltpu
from jax.sharding import PartitionSpec as P

B = 64
PAIR_DEV = 2
ITERS = 3
MOST_CHUNKS = 2
LANES = 128
ROWS = B * B // LANES
PAD = 32
STEP = 4


def deal_evenly(pair_slots, owner_count, each_owner):
    flat_slots = pair_slots.reshape(-1, 2)
    filled = (flat_slots[:, 0] >= 0).astype(jnp.int32)
    position = jnp.cumsum(filled, dtype=jnp.int32) - filled
    wanted = lax.broadcasted_iota(jnp.int32, (owner_count, each_owner), 1) * owner_count
    wanted = (wanted + lax.broadcasted_iota(jnp.int32, (owner_count, each_owner), 0)).reshape(-1)
    matched = (position[None, :] == wanted[:, None]) & (filled[None, :] == 1)
    picked = jnp.sum(jnp.where(matched[:, :, None], flat_slots[None], 0), axis=1)
    return picked.reshape(owner_count, each_owner, 2)


def gather_kernel(ids_ref, src_ref, *out_refs):
    count, terms = out_refs[0].shape[:2]
    for slot, out_ref in enumerate(out_refs):
        def pick(dest, unused, slot=slot, out_ref=out_ref):
            for term in range(terms):
                out_ref[dest, term] = src_ref[ids_ref[(slot * count + dest) * terms + term]]
            return unused

        lax.fori_loop(0, count, pick, 0)


def gather_pieces(ids, pieces, slots, count):
    norb, rows, lanes = pieces.shape
    block = max(8, rows // 4)
    return pl.pallas_call(
        gather_kernel,
        grid_spec=pltpu.PrefetchScalarGridSpec(
            num_scalar_prefetch=1,
            grid=(rows // block,),
            in_specs=[pl.BlockSpec((norb, block, lanes), lambda i, ids: (0, i, 0))],
            out_specs=[pl.BlockSpec((count, 2, block, lanes), lambda i, ids: (0, 0, i, 0))] * slots,
        ),
        out_shape=[jax.ShapeDtypeStruct((count, 2, rows, lanes), jnp.float32)] * slots,
        cost_estimate=pl.CostEstimate(flops=0, bytes_accessed=8 * norb * rows * lanes, transcendentals=0),
        name="pick_pieces",
    )(ids, pieces)


def scatter_kernel(ids_ref, *refs):
    out_ref = refs[-1]
    out_ref[...] = jnp.zeros_like(out_ref)
    count, terms = refs[0].shape[:2]
    for slot, in_ref in enumerate(refs[:-1]):
        def add(dest, unused, slot=slot, in_ref=in_ref):
            for term in range(terms):
                orbit = ids_ref[(slot * count + dest) * terms + term]
                out_ref[orbit] = out_ref[orbit] + in_ref[dest, term]
            return unused

        lax.fori_loop(0, count, add, 0)


def scatter_pieces(ids, parts, norb):
    count, terms, rows, lanes = parts[0].shape
    block = max(8, rows // 4)
    return pl.pallas_call(
        scatter_kernel,
        grid_spec=pltpu.PrefetchScalarGridSpec(
            num_scalar_prefetch=1,
            grid=(rows // block,),
            in_specs=[pl.BlockSpec((count, terms, block, lanes), lambda i, ids: (0, 0, i, 0))] * len(parts),
            out_specs=pl.BlockSpec((norb, block, lanes), lambda i, ids: (0, i, 0)),
        ),
        out_shape=jax.ShapeDtypeStruct((norb, rows, lanes), jnp.float32),
        cost_estimate=pl.CostEstimate(flops=0, bytes_accessed=8 * norb * rows * lanes, transcendentals=0),
        name="add_pieces",
    )(ids, *parts)


def lane_ids(shape):
    return lax.broadcasted_iota(jnp.int32, shape, len(shape) - 1)


def shift_plane(plane, off_y, off_z):
    shape = plane.shape
    lane = lane_ids(shape)
    row = lax.broadcasted_iota(jnp.int32, shape, 0)
    linear = off_y * B + off_z
    across = jnp.bitwise_and(linear, LANES - 1)
    down = jnp.right_shift(linear, 7)
    turned = pltpu.roll(plane, across, 1)
    near = pltpu.roll(turned, jnp.bitwise_and(down, ROWS - 1), 0)
    far = pltpu.roll(turned, jnp.bitwise_and(down + 1, ROWS - 1), 0)
    moved = jnp.where(lane >= across, near, far)
    from_y = row * 2 + jnp.right_shift(lane, 6) - off_y
    from_z = jnp.bitwise_and(lane, B - 1) - off_z
    inside = (from_y >= 0) & (from_y < B) & (from_z >= 0) & (from_z < B)
    return jnp.where(inside, moved, 0.0)


def operate_plane(before, plane, after):
    shape = plane.shape
    lane = lane_ids(shape)
    row = lax.broadcasted_iota(jnp.int32, shape, 0)
    z = jnp.bitwise_and(lane, B - 1)
    upper_z = jnp.where(z < B - 1, pltpu.roll(plane, LANES - 1, 1), 0.0)
    lower_z = jnp.where(z > 0, pltpu.roll(plane, 1, 1), 0.0)
    half = pltpu.roll(plane, B, 1)
    down = jnp.where(row > 0, pltpu.roll(half, 1, 0), 0.0)
    up = jnp.where(row < ROWS - 1, pltpu.roll(half, ROWS - 1, 0), 0.0)
    beside = (before + after) + (half + jnp.where(lane < B, down, up))
    return 6.0 * plane - beside - upper_z - lower_z


def fold(values):
    return jnp.sum(values.reshape(ROWS // 8, 8, LANES), axis=0)


def total(acc):
    return jnp.sum(acc, axis=(0, 1), keepdims=True)


def solve_kernel(info_ref, *refs):
    chunks = (len(refs) - 6) // 2
    in_refs, out_refs = refs[:chunks], refs[chunks : 2 * chunks]
    wide, partner, direction, resid, image, potential = refs[2 * chunks :]
    count, terms, rows, lanes = in_refs[0].shape
    each = rows // ROWS
    dx, dy, dz = info_ref[0], info_ref[1], info_ref[2]
    keep = jnp.where(info_ref[3] > 0, 1.0, 0.0).astype(jnp.float32)
    edge = jnp.zeros((PAD, ROWS, LANES), jnp.float32)
    wide[pl.ds(0, PAD)] = edge
    wide[pl.ds(PAD + B, PAD)] = edge
    direction[0] = edge[0]
    direction[B + 1] = edge[0]
    none = jnp.zeros((8, LANES), jnp.float32)

    def place(owner, chunk, i):
        return (owner * chunks + chunk) * each + i

    def load(owner, unused):
        for chunk in range(chunks):
            for i in range(each):
                wide[PAD + place(owner, chunk, i)] = in_refs[chunk][owner, 1, pl.ds(i * ROWS, ROWS)]
        return unused

    lax.fori_loop(0, count, load, 0)

    def start(owner, acc):
        for chunk in range(chunks):
            for i in range(each):
                x = place(owner, chunk, i)
                other = shift_plane(wide[PAD + x - dx], dy, dz)
                partner[x] = other
                density = in_refs[chunk][owner, 0, pl.ds(i * ROWS, ROWS)] * other
                direction[x + 1] = density
                resid[x] = density
                acc = acc + fold(density * density)
        return acc

    norm_now = total(lax.fori_loop(0, count, start, none))

    for turn in range(ITERS):
        def apply(block, acc):
            for i in range(STEP):
                x = block * STEP + i
                plane = direction[x + 1]
                result = operate_plane(direction[x], plane, direction[x + 2])
                image[x] = result
                acc = acc + fold(plane * result)
            return acc

        step_len = norm_now / total(lax.fori_loop(0, B // STEP, apply, none))

        if turn == ITERS - 1:
            break

        def advance(block, acc):
            for i in range(STEP):
                x = block * STEP + i
                moved = step_len * direction[x + 1]
                potential[x] = moved if turn == 0 else potential[x] + moved
                left = resid[x] - step_len * image[x]
                resid[x] = left
                acc = acc + fold(left * left)
            return acc

        norm_next = total(lax.fori_loop(0, B // STEP, advance, none))
        ratio = norm_next / norm_now

        def renew(block, unused):
            for i in range(STEP):
                x = block * STEP + i
                direction[x + 1] = resid[x] + ratio * direction[x + 1]
            return unused

        lax.fori_loop(0, B // STEP, renew, 0)
        norm_now = norm_next

    def finish(owner, unused):
        for chunk in range(chunks):
            for i in range(each):
                x = place(owner, chunk, i)
                found = (potential[x] + step_len * direction[x + 1]) * keep
                out_refs[chunk][owner, 0, pl.ds(i * ROWS, ROWS)] = found * partner[x]
                wide[PAD + x] = found * in_refs[chunk][owner, 0, pl.ds(i * ROWS, ROWS)]
        return unused

    lax.fori_loop(0, count, finish, 0)

    def give_back(owner, unused):
        for chunk in range(chunks):
            for i in range(each):
                x = place(owner, chunk, i)
                out_refs[chunk][owner, 1, pl.ds(i * ROWS, ROWS)] = shift_plane(wide[PAD + x + dx], -dy, -dz)
        return unused

    lax.fori_loop(0, count, give_back, 0)


def solve_pair(info, parts):
    box = (B, ROWS, LANES)
    vmem = pl.BlockSpec(memory_space=pltpu.VMEM)
    return pl.pallas_call(
        solve_kernel,
        in_specs=[pl.BlockSpec(memory_space=pltpu.SMEM)] + [vmem] * len(parts),
        out_specs=[vmem] * len(parts),
        out_shape=[jax.ShapeDtypeStruct(p.shape, jnp.float32) for p in parts],
        scratch_shapes=[
            pltpu.VMEM((B + 2 * PAD, ROWS, LANES), jnp.float32),
            pltpu.VMEM(box, jnp.float32),
            pltpu.VMEM((B + 2, ROWS, LANES), jnp.float32),
            pltpu.VMEM(box, jnp.float32),
            pltpu.VMEM(box, jnp.float32),
            pltpu.VMEM(box, jnp.float32),
        ],
        compiler_params=pltpu.CompilerParams(vmem_limit_bytes=32 * 1024 * 1024),
        cost_estimate=pl.CostEstimate(flops=0, bytes_accessed=40 * 1024 * 1024, transcendentals=0),
        name="solve_pair",
    )(info, *parts)


def swap_kernel(in_ref, out_ref, send_sems, recv_sems, own_sem):
    count = in_ref.shape[0]
    me = lax.axis_index("grid")
    barrier = pltpu.get_barrier_semaphore()
    for gap in range(1, count):
        pl.semaphore_signal(
            barrier,
            inc=1,
            device_id={"grid": lax.rem(me + gap, count)},
            device_id_type=pl.DeviceIdType.MESH,
        )
    pl.semaphore_wait(barrier, count - 1)
    copies = []
    for gap in range(1, count):
        peer = lax.rem(me + gap, count)
        copy = pltpu.make_async_remote_copy(
            src_ref=in_ref.at[peer],
            dst_ref=out_ref.at[me],
            send_sem=send_sems.at[gap - 1],
            recv_sem=recv_sems.at[gap - 1],
            device_id={"grid": peer},
            device_id_type=pl.DeviceIdType.MESH,
        )
        copy.start()
        copies.append(copy)
    own = pltpu.make_async_copy(in_ref.at[me], out_ref.at[me], own_sem)
    own.start()
    own.wait()
    for copy in copies:
        copy.wait()


def swap(parts, count):
    hbm = pl.BlockSpec(memory_space=pl.ANY)
    return pl.pallas_call(
        swap_kernel,
        in_specs=[hbm],
        out_specs=hbm,
        out_shape=jax.ShapeDtypeStruct(parts.shape, jnp.float32),
        scratch_shapes=[
            pltpu.SemaphoreType.DMA((count - 1,)),
            pltpu.SemaphoreType.DMA((count - 1,)),
            pltpu.SemaphoreType.DMA,
        ],
        compiler_params=pltpu.CompilerParams(collective_id=0, has_side_effects=True),
        cost_estimate=pl.CostEstimate(flops=0, bytes_accessed=80 * 1024 * 1024, transcendentals=0),
        name="swap_pieces",
    )(parts)


def exchange(parts, count, beside):
    if beside or count > 16:
        return lax.all_to_all(parts, "grid", split_axis=0, concat_axis=0, tiled=True)
    return swap(parts, count)


def body(orbitals, anchors, pair_slots):
    grid_count = lax.axis_size("grid")
    owner_count = lax.axis_size("grp") * grid_count
    group_idx = lax.axis_index("grp")
    place_idx = lax.axis_index("grid")
    assignment = deal_evenly(pair_slots, owner_count, PAIR_DEV)
    slots = assignment.shape[1]
    filled = assignment[..., 0] >= 0
    safe_ids = jnp.maximum(assignment, 0)
    group_table = lax.dynamic_slice_in_dim(safe_ids, group_idx * grid_count, grid_count, 0)
    ids = jnp.transpose(group_table, (1, 0, 2)).reshape(-1)
    owner_idx = group_idx * grid_count + place_idx
    own_pairs = safe_ids[owner_idx]
    offsets = anchors[own_pairs[:, 1]] - anchors[own_pairs[:, 0]]
    info = jnp.concatenate([offsets, filled[owner_idx].astype(jnp.int32)[:, None]], axis=1)

    norb_local, cells = orbitals.shape
    stacked = orbitals.reshape(norb_local, cells // LANES, LANES)
    chunks = math.gcd(MOST_CHUNKS, cells // (B * B))
    rows = stacked.shape[1] // chunks
    arrived = [[None] * chunks for _ in range(slots)]
    for chunk in range(chunks):
        pieces = lax.all_gather(stacked[:, chunk * rows : (chunk + 1) * rows], "grp", axis=0, tiled=True)
        outgoing = gather_pieces(ids, pieces, slots, grid_count)
        for slot in range(slots):
            arrived[slot][chunk] = exchange(outgoing[slot], grid_count, slot > 0)
    returned = []
    for slot in range(slots):
        terms = solve_pair(info[slot], arrived[slot])
        returned.append(
            [
                exchange(t, grid_count, slot < slots - 1 and chunk == 0)
                for chunk, t in enumerate(terms)
            ]
        )
    results = []
    for chunk in range(chunks):
        summed = scatter_pieces(ids, [r[chunk] for r in returned], anchors.shape[0])
        results.append(lax.psum_scatter(summed, "grp", scatter_dimension=0, tiled=True))
    return jnp.concatenate(results, axis=1).reshape(norb_local, cells)


def solution(mesh):
    return jax.shard_map(
        body,
        mesh=mesh,
        in_specs=(P("grp", "grid"), P(), P()),
        out_specs=P("grp", "grid"),
        check_vma=False,
    )
```
